32 devices in a mesh: vocab: 16 (over z, x, core), seq: 2 (over y).
Axes of the slice: x: 2, y: 2, z: 4, core: 2. Of those that a mesh axis runs over, the one named last changes fastest.
Arguments:
- hidden_states: bfloat16 [512, 3584], P('seq', 'vocab'), may hold values from -6 to 6
- norm_gain: float32 [3584], replicated, may hold values from 0.5 to 1.5
- embedding: bfloat16 [256000, 3584], P(('vocab', 'seq')), may hold values from -0.29882812 to 0.29882812
- targets: int32 [512], replicated, may hold values from 0 to 255999
Outputs:
- token_loss: float32 [512], P('seq')
- mean_loss: float32 [], replicated
The draws below stay inside these ranges and needn't reach their ends.
All inputs are finite; a program needn't handle non-finite values.
Results may differ from the reference program's by a relative error of at most 0.0005.
Values may be sent and summed in bfloat16 or wider, within the bound.
A program may use at most 128 MiB of HBM per device.

```python
import jax
import jax.numpy as jnp
from jax import lax

D = 3584
VOCAB = 256000
TOKENS = 512
N_VOCAB = 16


def place_ends(values, own_key, smallest, largest):
    longest = values.shape.index(max(values.shape))
    spots = []
    for shift in (0, 1):
        where = [jax.random.randint(jax.random.fold_in(own_key, axis), (), 0, length) for axis, length in enumerate(values.shape)]
        where[longest] = (where[longest] + shift) % values.shape[longest]
        spots.append(tuple(where))
    return values.at[spots[0]].set(smallest).at[spots[1]].set(largest)


def block_scale(key, shape, cuts, least, high):
    def one(dim, blocks):
        steps = jax.random.uniform(jax.random.fold_in(jax.random.fold_in(key, 6), dim), (blocks,), jnp.float32, least / len(cuts), high / len(cuts))
        return jnp.repeat(jnp.exp(steps), shape[dim] // blocks).reshape((-1,) + (1,) * (len(shape) - dim - 1))

    level = one(*cuts[0])
    for cut in cuts[1:]:
        level = level * one(*cut)
    return level


def scatter_about(rng, extent, deviation, reach, split=(), held_as=jnp.bfloat16):
    drawn = jax.random.normal(rng, extent, jnp.float32) * deviation
    if len(split) > 0:
        drawn = block_scale(rng, extent, split, -0.22, 0.18) * drawn
    return jnp.clip(drawn, min=-reach, max=reach).astype(held_as)


def setup_inputs(seed: int = 0) -> dict:
    seeds = jax.random.split(jax.random.key(seed), 5)
    return {
        "hidden_states": scatter_about(seeds[0], (TOKENS, D), 1.0, 6.0, ((0, 2), (1, 16))),
        "norm_gain": jnp.clip(1.0 + 0.1 * jax.random.normal(seeds[1], (D,), jnp.float32), 0.5, 1.5),
        "embedding": scatter_about(seeds[2], (VOCAB, D), (3.0 * D ** -0.5), 0.29882812, ((0, 32),)),
        "targets": place_ends(jax.random.randint(seeds[3], (TOKENS,), 0, VOCAB), jax.random.fold_in(seeds[3], 1), 0, VOCAB - 1).astype(jnp.int32),
    }


def reference(hidden_states, norm_gain, embedding, targets):
    values = hidden_states.astype(jnp.float32)
    meansq = lax.optimization_barrier(jnp.mean(values * values, axis=-1, keepdims=True))
    normed = (values * lax.rsqrt(meansq + 1e-06) * norm_gain).astype(jnp.bfloat16)
    block_rows = VOCAB // N_VOCAB
    blocks = embedding.reshape(N_VOCAB, block_rows, D)
    starts = jnp.arange(N_VOCAB, dtype=jnp.int32) * block_rows

    def visit(carry, inputs):
        total, picked = carry
        table, start = inputs
        scores = jnp.dot(table, normed.T, preferred_element_type=jnp.float32)
        capped = 30.0 * jnp.tanh(scores / 30.0)
        total = total + lax.optimization_barrier(jnp.sum(jnp.exp(capped), axis=0))
        ids = start + jnp.arange(block_rows, dtype=jnp.int32)
        hit = ids[:, None] == targets[None, :]
        picked = picked + lax.optimization_barrier(jnp.sum(jnp.where(hit, capped, 0.0), axis=0))
        return ((total, picked), None)
    zeros = jnp.zeros((TOKENS,), jnp.float32)
    (total, picked), unused = lax.scan(visit, (zeros, zeros), (blocks, starts))
    token_loss = jnp.log(total) - picked
    return (token_loss, jnp.mean(token_loss))
```

```python
import functools

import jax
import jax.numpy as jnp
from jax import lax
from jax.experimental import pallas as pl
from jax.experimental.pallas import tpu as pltpu
from jax.sharding import PartitionSpec as P

LANES = 128
SLOTS = 3
LOG2E = 1.4426950408889634


def tile_rows(rows, limit):
    best = rows
    for unit in (16, 8):
        sizes = [n for n in range(unit, limit + 1, unit) if rows % n == 0]
        if sizes:
            return max(sizes)
    return best


def kernel(cfg, ht_ref, gain_ref, targets_ref, emb_ref, loss_ref, mean_ref,
           raw, normed, acc, buf_a, buf_b, stat, rbuf, fin1, fin2, lossbuf, sums,
           z_send, z_recv, p_send, p_recv, c_send, c_recv, s_send, s_recv,
           f1_send, f1_recv, f2_send, f2_recv, own_sem, a_sem, b_sem):
    nv, ns, group, planes, width, own, tokens, rows, tm, features, sub = cfg
    v, s = lax.axis_index("vocab"), lax.axis_index("seq")
    p, q = v // group, v % group
    core = q % 2
    half = (group // 2) * ns
    hidx = (q // 2) * ns + s
    count = nv * ns
    me = s * nv + v
    gw = group * width
    tiles = rows // tm

    def plane_of(k):
        return (p + k) % planes

    def remote(src, dst, send, recv, vv, ss):
        return pltpu.make_async_remote_copy(
            src_ref=src, dst_ref=dst, send_sem=send, recv_sem=recv,
            device_id={"vocab": vv, "seq": ss},
            device_id_type=pl.DeviceIdType.MESH)

    first = planes - 2

    def a_copy(k, i, slot):
        col = pl.multiple_of(plane_of(k) * gw, LANES)
        row = pl.multiple_of(i * tm, 8)
        return pltpu.make_async_copy(
            emb_ref.at[pl.ds(row, tm), pl.ds(col, gw)], buf_a.at[slot], a_sem.at[slot])

    def b_copy(i, slot, part):
        col = pl.multiple_of(plane_of(first + part) * gw, LANES)
        row = pl.multiple_of(i * tm, 8)
        return pltpu.make_async_copy(
            emb_ref.at[pl.ds(row, tm), pl.ds(col, gw)],
            buf_b.at[slot, :, pl.ds(part * gw, gw)], b_sem.at[slot, part])

    total_a = first * tiles

    def a_start(n):
        for k in range(first):
            @pl.when((n >= k * tiles) & (n < (k + 1) * tiles))
            def _():
                a_copy(k, n - k * tiles, n % SLOTS).start()

    for n in range(min(SLOTS - 1, total_a)):
        a_copy(n // tiles, n % tiles, n % SLOTS).start()
    for n in range(min(SLOTS - 1, tiles)):
        for part in range(2):
            b_copy(n, n, part).start()

    h = ht_ref[...].astype(jnp.float32)
    stat[me] = jnp.sum(h * h, axis=0, keepdims=True)

    barrier = pltpu.get_barrier_semaphore()

    def greet(d, _):
        peer = (me + d) % count
        pl.semaphore_signal(barrier, inc=1,
                            device_id={"vocab": peer % nv, "seq": peer // nv},
                            device_id_type=pl.DeviceIdType.MESH)
        return 0

    lax.fori_loop(1, count, greet, 0)
    pl.semaphore_wait(barrier, count - 1)

    def tile_at(k, qq, ss):
        return raw.at[k, pl.ds(pl.multiple_of(qq * width, 16), width),
                      pl.ds(pl.multiple_of(ss * own, LANES), own)]

    def own_of(k):
        return ht_ref if k == 0 else tile_at(k, q, s)

    def z_copy(k):
        target = (p + planes - k) % planes
        return remote(ht_ref, tile_at(k, q, s), z_send.at[k], z_recv.at[k],
                      target * group + q, s)

    def p_copy(k, j):
        other = (hidx + j) % half
        return remote(own_of(k), tile_at(k, q, s), p_send.at[k, j], p_recv.at[k, j],
                      p * group + 2 * (other // ns) + core, other % ns)

    def c_copy(k, j):
        tile = (hidx + half - j) % half
        place = tile_at(k, 2 * (tile // ns) + core, tile % ns)
        return remote(place, place, c_send.at[k, j], c_recv.at[k, j],
                      p * group + (q + 1 - 2 * core), s)

    def c_own(k):
        return remote(own_of(k), tile_at(k, q, s), c_send.at[k, 0], c_recv.at[k, 0],
                      p * group + (q + 1 - 2 * core), s)

    def s_copy(d):
        peer = (me + d) % count
        return remote(stat.at[me], stat.at[me], s_send.at[d], s_recv.at[d],
                      peer % nv, peer // nv)

    def loop(low, high, action):
        def body(i, _):
            action(i)
            return 0
        lax.fori_loop(low, high, body, 0)

    def spread(k):
        loop(1, half, lambda j: p_copy(k, j).start())
        c_own(k).start()

    def relay(k):
        def one(j):
            p_copy(k, j).wait_recv()
            c_copy(k, j).start()
        loop(1, half, one)

    loop(1, count, lambda d: s_copy(d).start())
    spread(0)
    for k in range(1, planes):
        z_copy(k).start()
    own_copy = pltpu.make_async_copy(ht_ref, tile_at(0, q, s), own_sem)
    own_copy.start()

    loop(1, count, lambda d: s_copy(d).wait_recv())
    for t in range(ns):
        part = stat[t * nv:(t + 1) * nv]
        meansq = jnp.sum(part, axis=0) / features
        rbuf[:, t * own:(t + 1) * own] = lax.rsqrt(meansq + 1e-06)

    relay(0)

    def normalize(k):
        loop(0, half, lambda j: c_copy(k, j).wait_recv())
        for i in range(gw // LANES):
            row = plane_of(k) * (gw // LANES) + i
            gain = jnp.broadcast_to(gain_ref[pl.ds(row, 1), :], (LANES, LANES)).T
            for c in range(tokens // LANES):
                cols = slice(c * LANES, (c + 1) * LANES)
                values = raw[k, i * LANES:(i + 1) * LANES, cols].astype(jnp.float32)
                out = values * rbuf[:, cols] * gain
                normed[k * gw + i * LANES:k * gw + (i + 1) * LANES, cols] = (
                    out.astype(jnp.bfloat16))

    own_copy.wait()
    normalize(0)

    def step_a(k, i):
        n = k * tiles + i
        a_copy(k, i, n % SLOTS).wait()

        @pl.when(n + SLOTS - 1 < total_a)
        def _():
            a_start(n + SLOTS - 1)

        place = pl.ds(pl.multiple_of(i * tm, 8), tm)
        product = jnp.dot(buf_a[n % SLOTS], normed[k * gw:(k + 1) * gw, :],
                          preferred_element_type=jnp.float32)
        if k == 0:
            acc[place, :] = product
        else:
            acc[place, :] += product

    base = (v * ns + s) * rows

    def step_b(i):
        slot = i % SLOTS
        for part in range(2):
            b_copy(i, slot, part).wait()

        @pl.when(i + SLOTS - 1 < tiles)
        def _():
            for part in range(2):
                b_copy(i + SLOTS - 1, (i + SLOTS - 1) % SLOTS, part).start()

        total = sums[0:8, :]
        picked = sums[8:16, :]
        for m in range(tm // sub):
            place = pl.ds(pl.multiple_of(i * tm + m * sub, 8), sub)
            scores = jnp.dot(buf_b[slot, m * sub:(m + 1) * sub, :],
                             normed[first * gw:planes * gw, :],
                             preferred_element_type=jnp.float32)
            if first > 0:
                scores = scores + acc[place, :]
            bent = jnp.tanh(scores * (1.0 / 30.0))
            grown = jnp.exp2(bent * (30.0 * LOG2E))
            want = targets_ref[...] - (base + i * tm + m * sub)
            hit = lax.broadcasted_iota(jnp.int32, (sub, tokens), 0) == want
            mine = jnp.where(hit, bent, 0.0)
            total = total + jnp.sum(grown.reshape(sub // 8, 8, tokens), axis=0)
            picked = picked + jnp.sum(mine.reshape(sub // 8, 8, tokens), axis=0)
        sums[0:8, :] = total
        sums[8:16, :] = picked

    middle = tiles // 2

    def ready(k):
        if k < planes:
            z_copy(k).wait_recv()
            spread(k)

    sums[...] = jnp.zeros_like(sums)
    for k in range(first):
        nexts = [k + 1] if k + 1 < first else [k + 1, k + 2]
        for e in nexts:
            ready(e)
        loop(0, middle, functools.partial(step_a, k))
        for e in nexts:
            relay(e)
        loop(middle, tiles, functools.partial(step_a, k))
        for e in nexts:
            normalize(e)
    loop(0, tiles, step_b)

    fleet = group * ns
    pos = q * ns + s

    def f1_copy(d):
        other = (pos + d) % fleet
        return remote(fin1.at[pos], fin1.at[pos], f1_send.at[d], f1_recv.at[d],
                      p * group + other // ns, other % ns)

    def f2_copy(d):
        other = (p + d) % planes
        return remote(fin2.at[p], fin2.at[p], f2_send.at[d], f2_recv.at[d],
                      other * group + q, s)

    fin1[pos, 0:1, :] = jnp.sum(sums[0:8, :], axis=0, keepdims=True)
    fin1[pos, 1:2, :] = jnp.sum(sums[8:16, :], axis=0, keepdims=True)
    loop(1, fleet, lambda d: f1_copy(d).start())
    loop(1, fleet, lambda d: f1_copy(d).wait_recv())
    fin2[p] = jnp.sum(fin1[...], axis=0)
    loop(1, planes, lambda d: f2_copy(d).start())
    loop(1, planes, lambda d: f2_copy(d).wait_recv())
    both = jnp.sum(fin2[...], axis=0)
    losses = jnp.log(both[0:1, :]) - 30.0 * both[1:2, :]
    lossbuf[...] = losses
    mean_ref[...] = jnp.sum(losses, axis=1, keepdims=True) / tokens
    loss_ref[...] = lossbuf[:, pl.ds(pl.multiple_of(s * own, LANES), own)]

    loop(1, count, lambda d: s_copy(d).wait_send())
    for k in range(planes):
        if k > 0:
            z_copy(k).wait_send()
        loop(1, half, lambda j: p_copy(k, j).wait_send())
        loop(0, half, lambda j: c_copy(k, j).wait_send())
    loop(1, fleet, lambda d: f1_copy(d).wait_send())
    loop(1, planes, lambda d: f2_copy(d).wait_send())


def local(nv, ns, hidden_states, norm_gain, embedding, targets):
    own, width = hidden_states.shape
    rows, features = embedding.shape
    tokens = targets.shape[0]
    group = 2
    while (group * width) % LANES:
        group *= 2
    planes = nv // group
    gw = group * width
    tm = tile_rows(rows, 800)
    sub = tile_rows(tm, 400)
    half = (group // 2) * ns
    fleet = group * ns
    count = nv * ns
    cfg = (nv, ns, group, planes, width, own, tokens, rows, tm, features, sub)
    dma = pltpu.SemaphoreType.DMA
    vmem = pl.BlockSpec(memory_space=pltpu.VMEM)
    loss, mean = pl.pallas_call(
        functools.partial(kernel, cfg),
        out_shape=(jax.ShapeDtypeStruct((1, own), jnp.float32),
                   jax.ShapeDtypeStruct((1, 1), jnp.float32)),
        in_specs=[vmem, vmem, vmem, pl.BlockSpec(memory_space=pl.ANY)],
        out_specs=(vmem, vmem),
        scratch_shapes=[
            pltpu.VMEM((planes, gw, tokens), jnp.bfloat16),
            pltpu.VMEM((features, tokens), jnp.bfloat16),
            pltpu.VMEM((rows, tokens), jnp.float32),
            pltpu.VMEM((SLOTS, tm, gw), jnp.bfloat16),
            pltpu.VMEM((SLOTS, tm, 2 * gw), jnp.bfloat16),
            pltpu.VMEM((count, 1, own), jnp.float32),
            pltpu.VMEM((1, tokens), jnp.float32),
            pltpu.VMEM((fleet, 2, tokens), jnp.float32),
            pltpu.VMEM((planes, 2, tokens), jnp.float32),
            pltpu.VMEM((1, tokens), jnp.float32),
            pltpu.VMEM((16, tokens), jnp.float32),
            dma((planes,)), dma((planes,)),
            dma((planes, half)), dma((planes, half)),
            dma((planes, half)), dma((planes, half)),
            dma((count,)), dma((count,)),
            dma((fleet,)), dma((fleet,)),
            dma((planes,)), dma((planes,)),
            dma, dma((SLOTS,)), dma((SLOTS, 2)),
        ],
        compiler_params=pltpu.CompilerParams(
            collective_id=0, has_side_effects=True, vmem_limit_bytes=60 * 2**20),
    )(hidden_states.T, norm_gain.reshape(-1, LANES), targets.reshape(1, -1), embedding)
    return loss.reshape(own), mean.reshape(())


def solution(mesh):
    placed = (P("seq", "vocab"), P(), P(("vocab", "seq"), None), P())
    body = functools.partial(local, mesh.shape["vocab"], mesh.shape["seq"])
    return jax.shard_map(
        body, mesh=mesh, in_specs=placed, out_specs=(P("seq"), P()), check_vma=False
    )
```

```python
import functools

import jax
import jax.numpy as jnp
from jax import lax
from jax.experimental import pallas as pl
from jax.experimental.pallas import tpu as pltpu
from jax.sharding import PartitionSpec as P

LANES = 128
SLOTS = 3
LOG2E = 1.4426950408889634


def tile_rows(rows, limit):
    best = rows
    for unit in (16, 8):
        sizes = [n for n in range(unit, limit + 1, unit) if rows % n == 0]
        if sizes:
            return max(sizes)
    return best


def kernel(cfg, ht_ref, gain_ref, targets_ref, emb_ref, loss_ref, mean_ref,
           raw, normed, acc, buf_a, buf_b, gcol, stat, rbuf, fin, lossbuf, sums,
           z_send, z_recv, p_send, p_recv, c_send, c_recv, s_send, s_recv,
           f_send, f_recv, own_sem, a_sem, b_sem):
    nv, ns, group, planes, width, own, tokens, rows, tm, features, sub = cfg
    v, s = lax.axis_index("vocab"), lax.axis_index("seq")
    p, q = v // group, v % group
    core = q % 2
    half = (group // 2) * ns
    hidx = (q // 2) * ns + s
    count = nv * ns
    me = s * nv + v
    gw = group * width
    tiles = rows // tm

    def plane_of(k):
        return (p + k) % planes

    def remote(src, dst, send, recv, vv, ss):
        return pltpu.make_async_remote_copy(
            src_ref=src, dst_ref=dst, send_sem=send, recv_sem=recv,
            device_id={"vocab": vv, "seq": ss},
            device_id_type=pl.DeviceIdType.MESH)

    first = planes - 2

    def a_copy(k, i, slot):
        col = pl.multiple_of(plane_of(k) * gw, LANES)
        row = pl.multiple_of(i * tm, 8)
        return pltpu.make_async_copy(
            emb_ref.at[pl.ds(row, tm), pl.ds(col, gw)], buf_a.at[slot], a_sem.at[slot])

    def b_copy(i, slot, part):
        col = pl.multiple_of(plane_of(first + part) * gw, LANES)
        row = pl.multiple_of(i * tm, 8)
        return pltpu.make_async_copy(
            emb_ref.at[pl.ds(row, tm), pl.ds(col, gw)],
            buf_b.at[slot, :, pl.ds(part * gw, gw)], b_sem.at[slot, part])

    total_a = first * tiles

    def a_start(n):
        for k in range(first):
            @pl.when((n >= k * tiles) & (n < (k + 1) * tiles))
            def _():
                a_copy(k, n - k * tiles, n % SLOTS).start()

    for n in range(min(SLOTS - 1, total_a)):
        a_copy(n // tiles, n % tiles, n % SLOTS).start()
    for n in range(min(SLOTS - 1, tiles)):
        for part in range(2):
            b_copy(n, n, part).start()

    barrier = pltpu.get_barrier_semaphore()

    def greet(d, _):
        peer = (me + d) % count
        pl.semaphore_signal(barrier, inc=1,
                            device_id={"vocab": peer % nv, "seq": peer // nv},
                            device_id_type=pl.DeviceIdType.MESH)
        return 0

    lax.fori_loop(1, count, greet, 0)
    h = ht_ref[...].astype(jnp.float32)
    stat[me] = jnp.sum(h * h, axis=0, keepdims=True)

    for k in range(planes):
        for i in range(gw // LANES):
            row = plane_of(k) * (gw // LANES) + i
            gcol[k * gw + i * LANES:k * gw + (i + 1) * LANES, :] = jnp.broadcast_to(
                gain_ref[pl.ds(row, 1), :], (LANES, LANES)).T
    pl.semaphore_wait(barrier, count - 1)

    def tile_at(k, qq, ss):
        return raw.at[k, pl.ds(pl.multiple_of(qq * width, 16), width),
                      pl.ds(pl.multiple_of(ss * own, LANES), own)]

    def own_of(k):
        return ht_ref if k == 0 else tile_at(k, q, s)

    def z_copy(k):
        target = (p + planes - k) % planes
        return remote(ht_ref, tile_at(k, q, s), z_send.at[k], z_recv.at[k],
                      target * group + q, s)

    def p_copy(k, j):
        other = (hidx + j) % half
        return remote(own_of(k), tile_at(k, q, s), p_send.at[k, j], p_recv.at[k, j],
                      p * group + 2 * (other // ns) + core, other % ns)

    def c_copy(k, j):
        tile = (hidx + half - j) % half
        place = tile_at(k, 2 * (tile // ns) + core, tile % ns)
        return remote(place, place, c_send.at[k, j], c_recv.at[k, j],
                      p * group + (q + 1 - 2 * core), s)

    def c_own(k):
        return remote(own_of(k), tile_at(k, q, s), c_send.at[k, 0], c_recv.at[k, 0],
                      p * group + (q + 1 - 2 * core), s)

    def s_copy(d):
        peer = (me + d) % count
        return remote(stat.at[me], stat.at[me], s_send.at[d], s_recv.at[d],
                      peer % nv, peer // nv)

    def loop(low, high, action):
        def body(i, _):
            action(i)
            return 0
        lax.fori_loop(low, high, body, 0)

    def spread(k):
        loop(1, half, lambda j: p_copy(k, j).start())
        c_own(k).start()

    def relay(k):
        def one(j):
            p_copy(k, j).wait_recv()
            c_copy(k, j).start()
        loop(1, half, one)

    loop(1, count, lambda d: s_copy(d).start())
    spread(0)
    for k in range(1, planes):
        z_copy(k).start()
    own_copy = pltpu.make_async_copy(ht_ref, tile_at(0, q, s), own_sem)
    own_copy.start()

    loop(1, count, lambda d: s_copy(d).wait_recv())
    for t in range(ns):
        part = stat[t * nv:(t + 1) * nv]
        meansq = jnp.sum(part, axis=0) / features
        rbuf[:, t * own:(t + 1) * own] = lax.rsqrt(meansq + 1e-06)

    relay(0)

    def normalize(k):
        loop(0, half, lambda j: c_copy(k, j).wait_recv())
        for i in range(gw // LANES):
            gain = gcol[k * gw + i * LANES:k * gw + (i + 1) * LANES, :]
            for c in range(tokens // LANES):
                cols = slice(c * LANES, (c + 1) * LANES)
                values = raw[k, i * LANES:(i + 1) * LANES, cols].astype(jnp.float32)
                out = values * rbuf[:, cols] * gain
                normed[k * gw + i * LANES:k * gw + (i + 1) * LANES, cols] = (
                    out.astype(jnp.bfloat16))

    own_copy.wait()
    normalize(0)

    def step_a(k, i):
        n = k * tiles + i
        a_copy(k, i, n % SLOTS).wait()

        @pl.when(n + SLOTS - 1 < total_a)
        def _():
            a_start(n + SLOTS - 1)

        place = pl.ds(pl.multiple_of(i * tm, 8), tm)
        product = jnp.dot(buf_a[n % SLOTS], normed[k * gw:(k + 1) * gw, :],
                          preferred_element_type=jnp.float32)
        if k == 0:
            acc[place, :] = product
        else:
            acc[place, :] += product

    base = (v * ns + s) * rows

    def step_b(i):
        slot = i % SLOTS
        for part in range(2):
            b_copy(i, slot, part).wait()

        @pl.when(i + SLOTS - 1 < tiles)
        def _():
            for part in range(2):
                b_copy(i + SLOTS - 1, (i + SLOTS - 1) % SLOTS, part).start()

        total = sums[0:8, :]
        picked = sums[8:16, :]
        for m in range(tm // sub):
            place = pl.ds(pl.multiple_of(i * tm + m * sub, 8), sub)
            scores = jnp.dot(buf_b[slot, m * sub:(m + 1) * sub, :],
                             normed[first * gw:planes * gw, :],
                             preferred_element_type=jnp.float32)
            if first > 0:
                scores = scores + acc[place, :]
            bent = jnp.tanh(scores * (1.0 / 30.0))
            grown = jnp.exp2(bent * (30.0 * LOG2E))
            want = targets_ref[...] - (base + i * tm + m * sub)
            hit = lax.broadcasted_iota(jnp.int32, (sub, tokens), 0) == want
            mine = jnp.where(hit, bent, 0.0)
            total = total + jnp.sum(grown.reshape(sub // 8, 8, tokens), axis=0)
            picked = picked + jnp.sum(mine.reshape(sub // 8, 8, tokens), axis=0)
        sums[0:8, :] = total
        sums[8:16, :] = picked

    def ready(k):
        z_copy(k).wait_recv()
        spread(k)

    sums[...] = jnp.zeros_like(sums)
    ready(1)
    for k in range(first):
        nexts = [k + 1] if k + 1 < first else [k + 1, k + 2]
        events = []
        if k == 0:
            events += [((e - 1) * tiles // planes, ready, e) for e in range(2, planes)]
        marks = (6,) if len(nexts) == 1 else (4, 9)
        events += [(mark * tiles // 10, relay, e) for mark, e in zip(marks, nexts)]
        done = 0
        for at, action, e in sorted(events, key=lambda event: event[0]):
            if at > done:
                loop(done, at, functools.partial(step_a, k))
                done = at
            action(e)
        loop(done, tiles, functools.partial(step_a, k))
        for e in nexts:
            normalize(e)
    loop(0, tiles, step_b)

    def f_copy(d):
        peer = (me + d) % count
        return remote(fin.at[me], fin.at[me], f_send.at[d], f_recv.at[d],
                      peer % nv, peer // nv)

    fin[me, 0:1, :] = jnp.sum(sums[0:8, :], axis=0, keepdims=True)
    fin[me, 1:2, :] = jnp.sum(sums[8:16, :], axis=0, keepdims=True)
    loop(1, count, lambda d: f_copy(d).start())
    loop(1, count, lambda d: f_copy(d).wait_recv())
    both = jnp.sum(fin[...], axis=0)
    losses = jnp.log(both[0:1, :]) - 30.0 * both[1:2, :]
    lossbuf[...] = losses
    mean_ref[...] = jnp.sum(losses, axis=1, keepdims=True) / tokens
    loss_ref[...] = lossbuf[:, pl.ds(pl.multiple_of(s * own, LANES), own)]

    loop(1, count, lambda d: s_copy(d).wait_send())
    for k in range(planes):
        if k > 0:
            z_copy(k).wait_send()
        loop(1, half, lambda j: p_copy(k, j).wait_send())
        loop(0, half, lambda j: c_copy(k, j).wait_send())
    loop(1, count, lambda d: f_copy(d).wait_send())


def local(nv, ns, hidden_states, norm_gain, embedding, targets):
    own, width = hidden_states.shape
    rows, features = embedding.shape
    tokens = targets.shape[0]
    group = 2
    while (group * width) % LANES:
        group *= 2
    planes = nv // group
    gw = group * width
    tm = tile_rows(rows, 800)
    sub = tile_rows(tm, 200)
    half = (group // 2) * ns
    count = nv * ns
    cfg = (nv, ns, group, planes, width, own, tokens, rows, tm, features, sub)
    dma = pltpu.SemaphoreType.DMA
    vmem = pl.BlockSpec(memory_space=pltpu.VMEM)
    loss, mean = pl.pallas_call(
        functools.partial(kernel, cfg),
        out_shape=(jax.ShapeDtypeStruct((1, own), jnp.float32),
                   jax.ShapeDtypeStruct((1, 1), jnp.float32)),
        in_specs=[vmem, vmem, vmem, pl.BlockSpec(memory_space=pl.ANY)],
        out_specs=(vmem, vmem),
        scratch_shapes=[
            pltpu.VMEM((planes, gw, tokens), jnp.bfloat16),
            pltpu.VMEM((features, tokens), jnp.bfloat16),
            pltpu.VMEM((rows, tokens), jnp.float32),
            pltpu.VMEM((SLOTS, tm, gw), jnp.bfloat16),
            pltpu.VMEM((SLOTS, tm, 2 * gw), jnp.bfloat16),
            pltpu.VMEM((features, LANES), jnp.float32),
            pltpu.VMEM((count, 1, own), jnp.float32),
            pltpu.VMEM((1, tokens), jnp.float32),
            pltpu.VMEM((count, 2, tokens), jnp.float32),
            pltpu.VMEM((1, tokens), jnp.float32),
            pltpu.VMEM((16, tokens), jnp.float32),
            dma((planes,)), dma((planes,)),
            dma((planes, half)), dma((planes, half)),
            dma((planes, half)), dma((planes, half)),
            dma((count,)), dma((count,)),
            dma((count,)), dma((count,)),
            dma, dma((SLOTS,)), dma((SLOTS, 2)),
        ],
        compiler_params=pltpu.CompilerParams(
            collective_id=0, has_side_effects=True, vmem_limit_bytes=60 * 2**20),
    )(hidden_states.T, norm_gain.reshape(-1, LANES), targets.reshape(1, -1), embedding)
    return loss.reshape(own), mean.reshape(())


def solution(mesh):
    placed = (P("seq", "vocab"), P(), P(("vocab", "seq"), None), P())
    body = functools.partial(local, mesh.shape["vocab"], mesh.shape["seq"])
    return jax.shard_map(
        body, mesh=mesh, in_specs=placed, out_specs=(P("seq"), P()), check_vma=False
    )
```
